32 devices in a mesh: view: 8 (over z, y), tok: 2 (over x), obj: 2 (over core).
Axes of the slice: x: 2, y: 2, z: 4, core: 2. Of those that a mesh axis runs over, the one named last changes fastest.
Arguments:
- latents: bfloat16 [512, 8, 2, 1280], P('tok', 'view', 'obj'), parts along dimension 2, may hold values from -8 to 8
- query_weight: bfloat16 [1280, 1024], P(None, 'tok'), may hold values from -2 to 2
- key_weight: bfloat16 [1280, 1024], P(None, 'tok'), may hold values from -14 to 14
- value_weight: bfloat16 [1280, 1024], P(None, 'tok'), may hold values from -0.15625 to 0.15625
- output_weight: bfloat16 [1024, 1280], P('tok'), may hold values from -0.1875 to 0.1875
- value_units: bfloat16 [1280, 5120], P(None, 'tok'), may hold values from -0.15625 to 0.15625
- gate_units: bfloat16 [1280, 5120], P(None, 'tok'), may hold values from -0.15625 to 0.15625
- down_weight: bfloat16 [5120, 1280], P('tok'), may hold values from -0.078125 to 0.078125
Outputs:
- refined: bfloat16 [512, 8, 2, 1280], P('tok', 'view', 'obj'), parts along dimension 2
The draws below stay inside these ranges and needn't reach their ends.
There are 2 independent parts, one for each index of `obj`. The reference program is written for one: setup_inputs(seed, part) draws one part's arguments, and reference() takes and returns one part's arrays. A program takes and returns all parts, laid end to end along the dimension named above; an argument that names none is the same for every part. Nothing has to cross between parts.
All inputs are finite; a program needn't handle non-finite values.
Results may differ from the reference program's by a relative error of at most 0.012.
Values may be sent and summed in bfloat16 or wider, within the bound.
A program may use at most 128 MiB of HBM per device.

```python
import jax
import jax.numpy as jnp
from jax import lax

D = 1280
HS = 64
FF = 5120
HEADS = 16
LT = 512
BATCH = 1
VIEWS = 8
HD = 1024
N_TOK = 2


def base_matrix(key):
    drawn = jax.random.normal(jax.random.fold_in(key, 7), (D, HEADS * HS), jnp.float32)
    return jnp.clip(drawn, -4.5, 4.5) / D ** 0.5


def draw_query_weight(key, part):
    return (2.5 * base_matrix(key)).astype(jnp.bfloat16)


def draw_key_weight(key, part):
    drawn = jax.random.normal(jax.random.fold_in(key, 9), (D, HEADS * HS), jnp.float32)
    independent = jnp.clip(drawn, -4.5, 4.5) / D ** 0.5
    result = independent
    return result.astype(jnp.bfloat16)


def draw_latents(key, part):
    extent = (LT, VIEWS, BATCH, D)
    result = jnp.clip(jax.random.normal(jax.random.fold_in(key, 6), extent, jnp.float32), -6.0, 6.0)
    return result.astype(jnp.bfloat16)


def steps_of(stream_key, shape, cuts, low, high):
    level, own = 1.0, jax.random.fold_in(stream_key, 6)
    for position, blocks in cuts:
        steps = jnp.exp(jax.random.uniform(jax.random.fold_in(own, position), (blocks,), jnp.float32, low / len(cuts), high / len(cuts)))
        level = level * jnp.repeat(steps, shape[position] // blocks).reshape([-1 if axis == position else 1 for axis in range(len(shape))])
    return level


def centred(own_key, shape, scale, most, split=(), kind=jnp.bfloat16):
    loudness = steps_of(own_key, shape, split, -0.22, 0.18) if split else 1.0
    values = jax.random.normal(own_key, shape, jnp.float32) * scale * loudness
    return jnp.minimum(jnp.maximum(values, -most), most).astype(kind)


def setup_inputs(seed: int = 0, part: int = 0) -> dict:
    key_of = jax.random.split(jax.random.key(seed), 9)
    own_keys = jax.random.split(jax.random.fold_in(key_of[8], part), 9)
    return {
        "latents": draw_latents(jax.random.fold_in(jax.random.fold_in(key_of[8], part), 71), part),
        "query_weight": draw_query_weight(jax.random.fold_in(key_of[8], 71), part),
        "key_weight": draw_key_weight(jax.random.fold_in(key_of[8], 71), part),
        "value_weight": centred(key_of[3], (D, HD), D ** -0.5, 0.15625, ((1, 2),)),
        "output_weight": centred(key_of[4], (HD, D), HD ** -0.5, 0.1875, ((0, 2),)),
        "value_units": centred(key_of[5], (D, FF), D ** -0.5, 0.15625, ((1, 2),)),
        "gate_units": centred(key_of[6], (D, FF), D ** -0.5, 0.15625, ((1, 2),)),
        "down_weight": centred(key_of[7], (FF, D), FF ** -0.5, 0.078125, ((0, 2),)),
    }


epsilon = 1e-05

def normalize(stream):
    average = lax.optimization_barrier(jnp.mean(stream, -1, keepdims=True))
    centered = stream - average
    spread = lax.optimization_barrier(jnp.mean(centered * centered, -1, keepdims=True))
    return centered * lax.rsqrt(spread + epsilon)

def head_attention(triple):
    queries, key_block, value_block = triple
    length_all = queries.shape[0]
    block_rows = 512 if length_all % 512 == 0 else length_all
    factor = HS ** (-0.5)

    def one_block(picked):
        scores = jnp.dot(picked, key_block.T, preferred_element_type=jnp.float32) * factor
        highest = lax.optimization_barrier(jnp.max(scores, -1, keepdims=True))
        weights = jnp.exp(scores - highest)
        totals = lax.optimization_barrier(jnp.sum(weights, -1, keepdims=True))
        blended = jnp.dot(weights.astype(jnp.bfloat16), value_block, preferred_element_type=jnp.float32)
        return blended / totals
    shaped = queries.reshape(length_all // block_rows, block_rows, queries.shape[1])
    return lax.map(one_block, shaped).reshape(length_all, queries.shape[1])

def reference(latents, query_weight, key_weight, value_weight, output_weight, value_units, gate_units, down_weight):
    stream = latents.astype(jnp.float32)
    normed = normalize(stream).astype(jnp.bfloat16)
    queries = jnp.dot(normed, query_weight, preferred_element_type=jnp.float32).astype(jnp.bfloat16)
    keys_all = jnp.dot(normed, key_weight, preferred_element_type=jnp.float32).astype(jnp.bfloat16)
    values_all = jnp.dot(normed, value_weight, preferred_element_type=jnp.float32).astype(jnp.bfloat16)

    def to_heads(projected):
        flat = projected.reshape(LT * VIEWS, BATCH, HEADS, HS)
        return flat.transpose(1, 2, 0, 3).reshape(BATCH * HEADS, LT * VIEWS, HS)
    blended = lax.map(head_attention, (to_heads(queries), to_heads(keys_all), to_heads(values_all)))
    attended = blended.reshape(BATCH, HEADS, LT * VIEWS, HS).transpose(2, 0, 1, 3)
    attended = attended.reshape(LT, VIEWS, BATCH, HEADS * HS).astype(jnp.bfloat16)
    head_width = HEADS * HS // N_TOK

    def add_heads(counter, totals):
        offset = (counter * head_width).astype(jnp.int32)
        chosen = lax.dynamic_slice_in_dim(attended, offset, head_width, 3)
        rows_block = lax.dynamic_slice_in_dim(output_weight, offset, head_width, 0)
        partial_sum = jnp.dot(chosen, rows_block, preferred_element_type=jnp.float32)
        return totals + partial_sum.astype(jnp.bfloat16).astype(jnp.float32)
    attention_out = lax.fori_loop(0, N_TOK, add_heads, jnp.zeros(stream.shape, jnp.float32))
    middle = stream + attention_out
    normed_two = normalize(middle).astype(jnp.bfloat16)
    unit_width = FF // N_TOK

    def add_units(counter, totals):
        offset = (counter * unit_width).astype(jnp.int32)
        linear = jnp.dot(normed_two, lax.dynamic_slice_in_dim(value_units, offset, unit_width, 1), preferred_element_type=jnp.float32)
        gating = jnp.dot(normed_two, lax.dynamic_slice_in_dim(gate_units, offset, unit_width, 1), preferred_element_type=jnp.float32)
        hidden = (linear * jax.nn.gelu(gating)).astype(jnp.bfloat16)
        rows_block = lax.dynamic_slice_in_dim(down_weight, offset, unit_width, 0)
        partial_sum = jnp.dot(hidden, rows_block, preferred_element_type=jnp.float32)
        return totals + partial_sum.astype(jnp.bfloat16).astype(jnp.float32)
    feed_out = lax.fori_loop(0, N_TOK, add_units, jnp.zeros(stream.shape, jnp.float32))
    return (middle + feed_out).astype(jnp.bfloat16)
```

```python
import functools
import math

import jax
import jax.numpy as jnp
from jax import lax
from jax.experimental import pallas as pl
from jax.experimental.pallas import tpu as pltpu
from jax.sharding import PartitionSpec as P

HS = 64
ONES = 16
CHUNK = 256
MESH = pl.DeviceIdType.MESH
ANY = pl.BlockSpec(memory_space=pl.ANY)
F32, BF16 = jnp.float32, jnp.bfloat16


epsilon = 1e-05


def passed_along(block, axis, distance):
    devices = range(lax.axis_size(axis))
    route = [((i - distance) % len(devices), i) for i in devices]
    return lax.ppermute(block, axis, route)


def normalize(stream):
    average = jnp.mean(stream, -1, keepdims=True)
    centered = stream - average
    spread = jnp.mean(centered * centered, -1, keepdims=True)
    return centered * lax.rsqrt(spread + epsilon)


def gelu(v):
    return 0.5 * v * (1.0 + jnp.tanh(math.sqrt(2.0 / math.pi) * (v + 0.044715 * (v * v * v))))


def block_kernel(
    views,
    latents,
    query_weight,
    key_weight,
    value_weight,
    output_weight,
    value_units,
    gate_units,
    down_weight,
    out_ref,
    rows_in,
    wq,
    wk,
    wv,
    wo,
    vu,
    gu,
    dw,
    normed,
    send_q,
    send_kv,
    q_all,
    kv_all,
    keys,
    vals,
    scores_a,
    scores_b,
    staged,
    att,
    middle,
    hidden,
    part_own,
    part_out,
    part_in,
    load_sem,
    lat_sem,
    kv_sem,
    q_sem,
    wo_sem,
    att_sem,
    relay_sem,
    part_sem,
):
    view, tok, obj = lax.axis_index("view"), lax.axis_index("tok"), lax.axis_index("obj")
    other, twin = 1 - tok, 1 - obj
    rows = rows_in.shape[1]
    width = rows_in.shape[2]
    half_of = (tok, other)

    def load(number, source, target):
        return pltpu.make_async_copy(source, target, load_sem.at[number])

    loads = [
        load(0, latents, rows_in.at[0]),
        load(1, key_weight, wk),
        load(2, value_weight, wv),
        load(3, query_weight, wq),
        load(4, output_weight, wo.at[tok]),
        load(5, value_units, vu),
        load(6, gate_units, gu),
        load(7, down_weight, dw),
    ]
    for item in loads[:4]:
        item.start()

    barrier = pltpu.get_barrier_semaphore()
    for d in range(1, views):
        pl.semaphore_signal(
            barrier, inc=1, device_id={"view": lax.rem(view + d, views)}, device_id_type=MESH
        )
    pl.semaphore_signal(barrier, inc=1, device_id={"tok": other}, device_id_type=MESH)
    pl.semaphore_signal(barrier, inc=1, device_id={"obj": twin}, device_id_type=MESH)

    def remote(source, target, sems, index, device):
        return pltpu.make_async_remote_copy(
            src_ref=source,
            dst_ref=target,
            send_sem=sems.at[(0,) + index],
            recv_sem=sems.at[(1,) + index],
            device_id=device,
            device_id_type=MESH,
        )

    lat_copy = remote(rows_in.at[0], rows_in.at[1], lat_sem, (), {"tok": other})

    loads[0].wait()
    normed[...] = normalize(rows_in[0].astype(F32)).astype(BF16)
    pl.semaphore_wait(barrier, views + 1)
    lat_copy.start()

    far_first = sorted(range(1, views), key=lambda d: abs(d - views // 2))

    def kv_copy(slot, d):
        peer = lax.rem(view + d, views)
        return remote(
            send_kv.at[slot, peer], kv_all.at[slot, view], kv_sem, (slot, d), {"view": peer}
        )

    def q_copy(slot, d):
        peer = lax.rem(view + d, views)
        return remote(send_q.at[slot, peer], q_all.at[slot, view], q_sem, (slot, d), {"view": peer})

    def kv_arrival(slot, d):
        source = lax.rem(view - d + views, views)
        return remote(
            send_kv.at[slot, source], kv_all.at[slot, source], kv_sem, (slot, d), {"view": source}
        )

    def q_arrival(slot, d):
        source = lax.rem(view - d + views, views)
        return remote(
            send_q.at[slot, source], q_all.at[slot, source], q_sem, (slot, d), {"view": source}
        )

    def project(weight):
        return jnp.dot(normed[...], weight[...], preferred_element_type=F32)

    def turned(projected):
        return projected.astype(BF16).T.reshape(views, HS, rows)

    def spread_kv(slot):
        send_kv[slot, :, 0] = turned(project(wk))
        send_kv[slot, :, 1] = turned(project(wv))
        for d in far_first:
            kv_copy(slot, d).start()
        kv_all[slot, view] = send_kv[slot, view]

    def spread_q(slot):
        send_q[slot] = turned(project(wq) * (HS**-0.5 * math.log2(math.e)))
        for d in far_first:
            q_copy(slot, d).start()
        q_all[slot, view] = send_q[slot, view]

    loads[1].wait()
    loads[2].wait()
    spread_kv(0)
    loads[3].wait()
    for item in loads[4:]:
        item.start()
    spread_q(0)

    lat_copy.wait_recv()
    loads[4].wait()
    share = wo.shape[1] // 2
    mine, theirs = pl.ds(obj * share, share), pl.ds(twin * share, share)
    wo_across = remote(wo.at[tok, mine], wo.at[tok, mine], wo_sem, (0,), {"tok": other})
    wo_across.start()
    normed[...] = normalize(rows_in[1].astype(F32)).astype(BF16)
    spread_kv(1)
    spread_q(1)

    vals[:, :, HS:, :] = jnp.ones((2, views, ONES, rows), BF16)

    def prepare(slot):
        def one(d, carry):
            source = lax.rem(view - d + views, views)

            @pl.when(d > 0)
            def _():
                kv_arrival(slot, d).wait_recv()

            keys[slot, source] = kv_all[slot, source, 0].T
            vals[slot, source, :HS, :] = kv_all[slot, source, 1]
            return carry

        lax.fori_loop(0, views, one, 0)

    prepare(0)
    prepare(1)

    steps = 2 * views
    blocks = [(slot, number) for slot in range(2) for number in range(views)]

    def place(n):
        slot, turn = n // views, lax.rem(n, views) + 1
        return slot, turn, lax.rem(view + turn, views)

    def fetch_q(n):
        slot, turn, target = place(n)

        @pl.when(turn != views)
        def _():
            q_arrival(slot, views - turn).wait_recv()

    def att_copy(n):
        slot, turn, target = place(n)
        half = jnp.where(slot == 0, tok, other)
        return remote(
            staged.at[slot, target],
            att.at[half, tok, view],
            att_sem,
            (slot, turn),
            {"view": target},
        )

    def att_arrival(n):
        slot, turn, _ = place(n)
        half = jnp.where(slot == 0, tok, other)
        source = lax.rem(view - turn + views, views)
        return remote(
            staged.at[slot, source],
            att.at[half, tok, source],
            att_sem,
            (slot, turn),
            {"view": source},
        )

    def relay_copy(n):
        slot, turn, _ = place(n)
        half = jnp.where(slot == 0, tok, other)
        source = lax.rem(view - turn + views, views)
        return remote(
            att.at[half, tok, source],
            att.at[half, tok, source],
            relay_sem,
            (slot, turn),
            {"tok": other},
        )

    def relay_arrival(n):
        slot, turn, _ = place(n)
        half = jnp.where(slot == 0, other, tok)
        source = lax.rem(view - turn + views, views)
        return remote(
            att.at[half, other, source],
            att.at[half, other, source],
            relay_sem,
            (slot, turn),
            {"tok": other},
        )

    def score(n, buffer, number):
        slot, turn, target = place(n)
        found = jnp.dot(
            keys[blocks[number]], q_all[slot, target], preferred_element_type=F32
        )
        buffer[number] = found
        return jnp.max(found, 0, keepdims=True)

    def blend(buffer, highest, number):
        weights = jnp.exp2(buffer[number] - highest).astype(BF16)
        return jnp.dot(vals[blocks[number]], weights, preferred_element_type=F32)

    def unit(n, current, highest, following):
        blended = jnp.zeros((HS + ONES, rows), F32)
        upcoming = jnp.full((1, rows), -1e30, F32)
        for number in range(steps):
            if following is not None:
                upcoming = jnp.maximum(upcoming, score(n + 1, following, number))
            blended = blended + blend(current, highest, number)
        result = (blended[:HS] / blended[HS : HS + 1]).astype(BF16)
        slot, turn, target = place(n)
        staged[slot, target] = result
        return upcoming

    def post(n):
        slot, turn, target = place(n)
        half = jnp.where(slot == 0, tok, other)

        @pl.when(turn != views)
        def _():
            att_copy(n).start()

        @pl.when(turn == views)
        def _():
            att[half, tok, view] = staged[slot, view]

    def relay(n):
        slot, turn, target = place(n)

        @pl.when(turn != views)
        def _():
            att_arrival(n).wait_recv()

        relay_copy(n).start()

    def first_scores():
        fetch_q(0)
        highest = jnp.full((1, rows), -1e30, F32)
        for number in range(steps):
            highest = jnp.maximum(highest, score(0, scores_a, number))
        return highest

    LAG = 2

    def two_steps(i, highest):
        n = 2 * i
        fetch_q(n + 1)
        highest = unit(n, scores_a, highest, scores_b)
        post(n)

        @pl.when(n >= LAG)
        def _():
            relay(n - LAG)

        fetch_q(n + 2)
        highest = unit(n + 1, scores_b, highest, scores_a)
        post(n + 1)

        @pl.when(n + 1 >= LAG)
        def _():
            relay(n + 1 - LAG)

        return highest

    highest = first_scores()
    highest = lax.fori_loop(0, views - 1, two_steps, highest)
    last = steps - 2
    fetch_q(last + 1)
    highest = unit(last, scores_a, highest, scores_b)
    post(last)
    relay(last - LAG)
    wo_arrival = remote(wo.at[other, mine], wo.at[other, mine], wo_sem, (0,), {"tok": other})
    wo_arrival.wait_recv()
    wo_swap = remote(wo.at[other, mine], wo.at[other, mine], wo_sem, (1,), {"obj": twin})
    wo_swap.start()
    unit(last + 1, scores_b, highest, None)
    post(last + 1)
    relay(last + 1 - LAG)
    relay(last)
    relay(last + 1)

    remote(wo.at[other, theirs], wo.at[other, theirs], wo_sem, (1,), {"obj": twin}).wait_recv()

    columns = width // CHUNK

    def join(slot):
        half = half_of[slot]
        gathered = att[half].reshape(2 * views * HS, rows).T

        def one(c, carry):
            at = pl.ds(pl.multiple_of(c * CHUNK, CHUNK), CHUNK)
            whole = wo[:, :, at].reshape(2 * views * HS, CHUNK)
            middle[slot, :, at] = rows_in[slot, :, at].astype(F32) + jnp.dot(
                gathered, whole, preferred_element_type=F32
            )
            return carry

        lax.fori_loop(0, columns, one, 0)
        normed[...] = normalize(middle[slot]).astype(BF16)

    def units():
        wide = 2 * CHUNK

        def one(c, carry):
            at = pl.ds(pl.multiple_of(c * wide, wide), wide)
            block = normed[...]
            linear = jnp.dot(block, vu[:, at], preferred_element_type=F32)
            gating = jnp.dot(block, gu[:, at], preferred_element_type=F32)
            hidden[:, at] = (linear * gelu(gating)).astype(BF16)
            return carry

        lax.fori_loop(0, hidden.shape[1] // wide, one, 0)

    def down(c):
        at = pl.ds(pl.multiple_of(c * CHUNK, CHUNK), CHUNK)
        return jnp.dot(hidden[...], dw[:, at], preferred_element_type=F32)

    def part_copy(c):
        return remote(part_out.at[c], part_in.at[c], part_sem, (c,), {"tok": other})

    def wait_relays(first):
        def one(n, carry):
            relay_arrival(first + n).wait_recv()
            return carry

        lax.fori_loop(0, views, one, 0)

    wait_relays(0)
    join(1)
    for item in loads[5:]:
        item.wait()
    units()

    def send_part(c, carry):
        part_out[c] = down(c).astype(BF16)
        part_copy(c).start()
        return carry

    lax.fori_loop(0, columns, send_part, 0)
    wait_relays(views)
    join(0)
    units()

    def keep_part(c, carry):
        part_own[c] = down(c)
        return carry

    lax.fori_loop(0, columns, keep_part, 0)

    for c in range(columns):
        part_copy(c).wait_recv()
        at = slice(c * CHUNK, (c + 1) * CHUNK)
        total = middle[0, :, at] + part_own[c] + part_in[c].astype(F32)
        out_ref[:, at] = total.astype(BF16)

    lat_copy.wait_send()
    wo_across.wait_send()
    wo_swap.wait_send()

    def drain(d, carry):
        for slot in range(2):
            kv_copy(slot, d).wait_send()
            q_copy(slot, d).wait_send()
            att_copy(slot * views + d - 1).wait_send()
        return carry

    lax.fori_loop(1, views, drain, 0)

    def drain_relays(n, carry):
        relay_copy(n).wait_send()
        return carry

    lax.fori_loop(0, steps, drain_relays, 0)

    def drain_parts(c, carry):
        part_copy(c).wait_send()
        return carry

    lax.fori_loop(0, columns, drain_parts, 0)


def by_heads(latents, *weights):
    views = lax.axis_size("view")
    width = latents.shape[-1]
    stream = latents.reshape(-1, width)
    rows = stream.shape[0]
    head_width, units = weights[0].shape[1], weights[4].shape[1]
    columns = width // CHUNK
    half = (2, views)
    dma = pltpu.SemaphoreType.DMA
    scratch = [
        pltpu.VMEM((2, rows, width), BF16),
        pltpu.VMEM((width, head_width), BF16),
        pltpu.VMEM((width, head_width), BF16),
        pltpu.VMEM((width, head_width), BF16),
        pltpu.VMEM((2, head_width, width), BF16),
        pltpu.VMEM((width, units), BF16),
        pltpu.VMEM((width, units), BF16),
        pltpu.VMEM((units, width), BF16),
        pltpu.VMEM((rows, width), BF16),
        pltpu.VMEM(half + (HS, rows), BF16),
        pltpu.VMEM(half + (2, HS, rows), BF16),
        pltpu.VMEM(half + (HS, rows), BF16),
        pltpu.VMEM(half + (2, HS, rows), BF16),
        pltpu.VMEM(half + (rows, HS), BF16),
        pltpu.VMEM(half + (HS + ONES, rows), BF16),
        pltpu.VMEM((2 * views, rows, rows), F32),
        pltpu.VMEM((2 * views, rows, rows), F32),
        pltpu.VMEM(half + (HS, rows), BF16),
        pltpu.VMEM((2, 2, views, HS, rows), BF16),
        pltpu.VMEM((2, rows, width), F32),
        pltpu.VMEM((rows, units), BF16),
        pltpu.VMEM((columns, rows, CHUNK), F32),
        pltpu.VMEM((columns, rows, CHUNK), BF16),
        pltpu.VMEM((columns, rows, CHUNK), BF16),
        dma((8,)),
        dma((2,)),
        dma((2, 2, views)),
        dma((2, 2, views)),
        dma((2, 2)),
        dma((2, 2, views + 1)),
        dma((2, 2, views + 1)),
        dma((2, columns)),
    ]
    result = pl.pallas_call(
        functools.partial(block_kernel, views),
        out_shape=jax.ShapeDtypeStruct((rows, width), BF16),
        in_specs=[ANY] * 8,
        out_specs=pl.BlockSpec(memory_space=pltpu.VMEM),
        scratch_shapes=scratch,
        compiler_params=pltpu.CompilerParams(
            collective_id=0, has_side_effects=True, vmem_limit_bytes=62 * 1024 * 1024
        ),
        name="block",
    )(stream, *weights)
    return result.reshape(latents.shape)


def by_ring(
    latents,
    query_weight,
    key_weight,
    value_weight,
    output_weight,
    value_units,
    gate_units,
    down_weight,
):
    stream = latents.astype(jnp.float32)
    normed = normalize(stream).astype(jnp.bfloat16)
    joined = jnp.concatenate([query_weight, key_weight, value_weight], 1)
    projected = jnp.dot(
        lax.all_gather(normed, "tok", axis=0, tiled=True),
        joined,
        preferred_element_type=jnp.float32,
    ).astype(jnp.bfloat16)
    head_width = query_weight.shape[1]
    queries = projected[..., :head_width]
    key_part = projected[..., head_width : 2 * head_width]
    value_part = projected[..., 2 * head_width :]
    length_all, local_views, objects = (queries.shape[0], queries.shape[1], queries.shape[2])
    head_count = head_width // HS
    query_rows = length_all * local_views
    queries_flat = queries.reshape(query_rows, objects, head_count, HS)
    factor = HS ** (-0.5)

    def attend(states, key_block, value_block):
        key_rows = key_block.shape[0]

        def one_view(counter, inner):
            highest, totals, blended = inner
            key_view = lax.dynamic_index_in_dim(key_block, counter, 1, keepdims=False).reshape(
                key_rows, objects, head_count, HS
            )
            value_view = lax.dynamic_index_in_dim(value_block, counter, 1, keepdims=False).reshape(
                key_rows, objects, head_count, HS
            )
            scores = (
                jnp.einsum(
                    "ibhe,jbhe->bhij", queries_flat, key_view, preferred_element_type=jnp.float32
                )
                * factor
            )
            newest = jnp.maximum(highest, jnp.max(scores, -1))
            shrink = jnp.exp(highest - newest)
            weights = jnp.exp(scores - newest[..., None])
            totals = totals * shrink + jnp.sum(weights, -1)
            update = jnp.einsum(
                "bhij,jbhe->bhie",
                weights.astype(jnp.bfloat16),
                value_view,
                preferred_element_type=jnp.float32,
            )
            blended = blended * shrink[..., None] + update
            return (newest, totals, blended)

        return lax.fori_loop(0, key_block.shape[1], one_view, states)

    start_state = (
        jnp.full((objects, head_count, query_rows), -1e30, jnp.float32),
        jnp.zeros((objects, head_count, query_rows), jnp.float32),
        jnp.zeros((objects, head_count, query_rows, HS), jnp.float32),
    )
    stacked = jnp.stack([key_part, value_part])
    states = attend(start_state, key_part, value_part)

    def rotate(counter, bundle):
        inner, buffer_kv = bundle
        buffer_kv = passed_along(buffer_kv, "view", 1)
        return (attend(inner, buffer_kv[0], buffer_kv[1]), buffer_kv)

    states, stacked = lax.fori_loop(0, lax.axis_size("view") - 1, rotate, (states, stacked))
    highest, totals, blended = states
    attended = (blended / totals[..., None]).transpose(2, 0, 1, 3)
    attended = attended.reshape(length_all, local_views, objects, head_width).astype(jnp.bfloat16)
    full_output = lax.all_gather(output_weight, "tok", axis=0, tiled=True)
    own_rows = lax.all_to_all(attended, "tok", split_axis=0, concat_axis=3, tiled=True)
    groups = lax.axis_size("tok")
    grouped = own_rows.reshape(
        own_rows.shape[0], own_rows.shape[1], own_rows.shape[2], groups, head_width
    )
    weight_groups = full_output.reshape(groups, head_width, full_output.shape[1])
    group_parts = jnp.einsum(
        "rvbgc,gcd->rvbgd", grouped, weight_groups, preferred_element_type=jnp.float32
    ).astype(jnp.bfloat16)
    attention_out = jnp.sum(group_parts.astype(jnp.float32), 3)
    middle = stream + attention_out
    normed_two = normalize(middle).astype(jnp.bfloat16)
    gathered = lax.all_gather(normed_two, "tok", axis=0, tiled=True)
    linear = jnp.dot(gathered, value_units, preferred_element_type=jnp.float32)
    gating = jnp.dot(gathered, gate_units, preferred_element_type=jnp.float32)
    hidden = (linear * jax.nn.gelu(gating)).astype(jnp.bfloat16)
    feed_out = lax.psum_scatter(
        jnp.dot(hidden, down_weight, preferred_element_type=jnp.float32).astype(jnp.bfloat16),
        "tok",
        scatter_dimension=0,
        tiled=True,
    ).astype(jnp.float32)
    return (middle + feed_out).astype(jnp.bfloat16)


def on_device(latents, query_weight, *weights):
    rows, width = latents.shape[0], latents.shape[-1]
    head_width, unit_width = query_weight.shape[1], weights[3].shape[1]
    fits = (
        latents.shape[1] == 1
        and latents.shape[2] == 1
        and head_width == lax.axis_size("view") * HS
        and lax.axis_size("tok") == 2
        and lax.axis_size("obj") == 2
        and rows == CHUNK
        and width % CHUNK == 0
        and unit_width % (2 * CHUNK) == 0
    )
    if fits:
        return by_heads(latents, query_weight, *weights)
    return by_ring(latents, query_weight, *weights)


def solution(mesh):
    return jax.shard_map(
        on_device,
        mesh=mesh,
        in_specs=(
            P("tok", "view", "obj", None),
            P(None, "tok"),
            P(None, "tok"),
            P(None, "tok"),
            P("tok", None),
            P(None, "tok"),
            P(None, "tok"),
            P("tok", None),
        ),
        out_specs=P("tok", "view", "obj", None),
        check_vma=False,
    )
```

```python
import functools
import math

import jax
import jax.numpy as jnp
from jax import lax
from jax.experimental import pallas as pl
from jax.experimental.pallas import tpu as pltpu
from jax.sharding import PartitionSpec as P

HS = 64
ONES = 16
CHUNK = 256
SUB = 128
LAG = 6
MESH = pl.DeviceIdType.MESH
ANY = pl.BlockSpec(memory_space=pl.ANY)
F32, BF16 = jnp.float32, jnp.bfloat16


epsilon = 1e-05


def passed_along(block, axis, distance):
    devices = range(lax.axis_size(axis))
    route = [((i - distance) % len(devices), i) for i in devices]
    return lax.ppermute(block, axis, route)


def normalize(stream):
    average = jnp.mean(stream, -1, keepdims=True)
    centered = stream - average
    spread = jnp.mean(centered * centered, -1, keepdims=True)
    return centered * lax.rsqrt(spread + epsilon)


def gelu(v):
    return 0.5 * v * (1.0 + jnp.tanh(math.sqrt(2.0 / math.pi) * (v + 0.044715 * (v * v * v))))


def block_kernel(
    views,
    latents,
    query_weight,
    key_weight,
    value_weight,
    output_weight,
    value_units,
    gate_units,
    down_weight,
    out_ref,
    rows_in,
    wq,
    wk,
    wv,
    wo,
    vu,
    gu,
    dw,
    normed,
    send_q,
    send_kv,
    q_all,
    kv_all,
    keys,
    vals,
    scores_a,
    scores_b,
    staged,
    att,
    gathered,
    middle,
    hidden,
    part_own,
    part_out,
    part_in,
    load_sem,
    lat_sem,
    kv_sem,
    q_sem,
    wo_sem,
    att_sem,
    relay_sem,
    part_sem,
):
    view, tok, obj = lax.axis_index("view"), lax.axis_index("tok"), lax.axis_index("obj")
    other, twin = 1 - tok, 1 - obj
    width = rows_in.shape[2]
    rows = 2 * SUB
    half_of = (tok, other)
    first, second = pl.ds(0, SUB), pl.ds(SUB, SUB)
    sub = (first, second)

    def load(number, source, target):
        return pltpu.make_async_copy(source, target, load_sem.at[number])

    loads = [
        load(0, latents.at[first], rows_in.at[0, first]),
        load(1, latents.at[second], rows_in.at[0, second]),
        load(2, key_weight, wk),
        load(3, value_weight, wv),
        load(4, query_weight, wq),
        load(5, output_weight, wo.at[tok]),
        load(6, value_units, vu),
        load(7, gate_units, gu),
        load(8, down_weight, dw),
    ]
    for item in loads[:5]:
        item.start()

    barrier = pltpu.get_barrier_semaphore()
    for d in range(1, views):
        pl.semaphore_signal(
            barrier, inc=1, device_id={"view": lax.rem(view + d, views)}, device_id_type=MESH
        )
    pl.semaphore_signal(barrier, inc=1, device_id={"tok": other}, device_id_type=MESH)
    pl.semaphore_signal(barrier, inc=1, device_id={"obj": twin}, device_id_type=MESH)

    def remote(source, target, sems, index, device):
        return pltpu.make_async_remote_copy(
            src_ref=source,
            dst_ref=target,
            send_sem=sems.at[(0,) + index],
            recv_sem=sems.at[(1,) + index],
            device_id=device,
            device_id_type=MESH,
        )

    lat_copies = [
        remote(rows_in.at[0, sub[ab]], rows_in.at[1, sub[ab]], lat_sem, (ab,), {"tok": other})
        for ab in range(2)
    ]
    far_first = sorted(range(1, views), key=lambda d: abs(d - views // 2))

    def kv_copy(chunk, d):
        peer = lax.rem(view + d, views)
        return remote(
            send_kv.at[chunk, peer], kv_all.at[chunk, view], kv_sem, (chunk, d), {"view": peer}
        )

    def q_copy(slot, ab, d):
        peer, chunk = lax.rem(view + d, views), 2 * slot + ab
        return remote(
            send_q.at[chunk, peer],
            q_all.at[ab, view, half_of[slot]],
            q_sem,
            (chunk, d),
            {"view": peer},
        )

    def kv_arrival(chunk, d):
        source = lax.rem(view - d + views, views)
        return remote(
            send_kv.at[chunk, source], kv_all.at[chunk, source], kv_sem, (chunk, d), {"view": source}
        )

    def q_arrival(slot, ab, d):
        source, chunk = lax.rem(view - d + views, views), 2 * slot + ab
        return remote(
            send_q.at[chunk, source],
            q_all.at[ab, source, half_of[slot]],
            q_sem,
            (chunk, d),
            {"view": source},
        )

    def level(slot, ab):
        normed[2 * slot + ab] = normalize(rows_in[slot, sub[ab]].astype(F32)).astype(BF16)

    def project(chunk, weight):
        return jnp.dot(normed[chunk], weight[...], preferred_element_type=F32)

    def turned(projected):
        return projected.astype(BF16).T.reshape(views, HS, SUB)

    def spread_kv(chunk):
        send_kv[chunk, :, 0] = turned(project(chunk, wk))
        send_kv[chunk, :, 1] = turned(project(chunk, wv))
        for d in far_first:
            kv_copy(chunk, d).start()
        kv_all[chunk, view] = send_kv[chunk, view]

    def make_q(chunk):
        send_q[chunk] = turned(project(chunk, wq) * (HS**-0.5 * math.log2(math.e)))

    def spread_q(slot, ab):
        for d in far_first:
            q_copy(slot, ab, d).start()
        q_all[ab, view, half_of[slot]] = send_q[2 * slot + ab, view]

    loads[0].wait()
    level(0, 0)
    loads[1].wait()
    pl.semaphore_wait(barrier, views + 1)
    for item in lat_copies:
        item.start()
    loads[2].wait()
    loads[3].wait()
    spread_kv(0)
    level(0, 1)
    spread_kv(1)
    loads[4].wait()
    for item in loads[5:]:
        item.start()
    make_q(0)
    make_q(1)

    lat_copies[0].wait_recv()
    level(1, 0)
    spread_kv(2)
    make_q(2)
    lat_copies[1].wait_recv()
    loads[5].wait()
    share = wo.shape[1] // 2
    mine, theirs = pl.ds(obj * share, share), pl.ds(twin * share, share)
    wo_across = remote(wo.at[tok, mine], wo.at[tok, mine], wo_sem, (0,), {"tok": other})
    wo_across.start()
    level(1, 1)
    spread_kv(3)
    spread_q(0, 0)
    spread_q(1, 0)
    make_q(3)
    spread_q(0, 1)
    spread_q(1, 1)

    vals[:, :, HS:, :] = jnp.ones((2, views, ONES, rows), BF16)

    def prepare(slot, ab):
        chunk = 2 * slot + ab

        def one(d, carry):
            source = lax.rem(view - d + views, views)

            @pl.when(d > 0)
            def _():
                kv_arrival(chunk, d).wait_recv()

            keys[slot, source, sub[ab]] = kv_all[chunk, source, 0].T
            vals[slot, source, :HS, sub[ab]] = kv_all[chunk, source, 1]
            return carry

        lax.fori_loop(0, views, one, 0)

    for chunk in range(4):
        prepare(chunk // 2, chunk % 2)

    steps = 2 * views
    blocks = [(slot, number) for slot in range(2) for number in range(views)]

    def place(n):
        ab, turn = n // views, lax.rem(n, views) + 1
        return ab, turn, lax.rem(view + turn, views), lax.rem(view - turn + views, views)

    def fetch_q(n):
        ab, turn, target, _ = place(n)

        @pl.when(turn != views)
        def _():
            for slot in range(2):
                q_arrival(slot, ab, views - turn).wait_recv()

    def att_copy(n):
        ab, turn, target, _ = place(n)
        return remote(
            staged.at[ab, target], att.at[ab, tok, view], att_sem, (ab, turn), {"view": target}
        )

    def att_arrival(n):
        ab, turn, _, source = place(n)
        return remote(
            staged.at[ab, source], att.at[ab, tok, source], att_sem, (ab, turn), {"view": source}
        )

    def relay_copy(n):
        ab, turn, _, source = place(n)
        block = att.at[ab, tok, source]
        return remote(block, block, relay_sem, (ab, turn), {"tok": other})

    def relay_arrival(n):
        ab, turn, _, source = place(n)
        block = att.at[ab, other, source]
        return remote(block, block, relay_sem, (ab, turn), {"tok": other})

    def score(n, buffer, number):
        ab, _, target, _ = place(n)
        queries = jnp.concatenate([q_all[ab, target, 0], q_all[ab, target, 1]], 1)
        found = jnp.dot(keys[blocks[number]], queries, preferred_element_type=F32)
        buffer[number] = found
        return jnp.max(found, 0, keepdims=True)

    def blend(buffer, highest, number):
        weights = jnp.exp2(buffer[number] - highest).astype(BF16)
        return jnp.dot(vals[blocks[number]], weights, preferred_element_type=F32)

    def unit(n, current, highest, following):
        blended = jnp.zeros((HS + ONES, rows), F32)
        upcoming = jnp.full((1, rows), -1e30, F32)
        for number in range(steps):
            if following is not None:
                upcoming = jnp.maximum(upcoming, score(n + 1, following, number))
            blended = blended + blend(current, highest, number)
        result = (blended[:HS] / blended[HS : HS + 1]).astype(BF16)
        ab, _, target, _ = place(n)
        staged[ab, target, 0] = result[:, :SUB]
        staged[ab, target, 1] = result[:, SUB:]
        return upcoming

    def post(n):
        ab, turn, target, _ = place(n)

        @pl.when(turn != views)
        def _():
            att_copy(n).start()

        @pl.when(turn == views)
        def _():
            att[ab, tok, view] = staged[ab, view]

    def relay(n):
        _, turn, _, _ = place(n)

        @pl.when(turn != views)
        def _():
            att_arrival(n).wait_recv()

        relay_copy(n).start()

    def first_scores():
        fetch_q(0)
        highest = jnp.full((1, rows), -1e30, F32)
        for number in range(steps):
            highest = jnp.maximum(highest, score(0, scores_a, number))
        return highest

    def two_steps(i, highest):
        n = 2 * i
        fetch_q(n + 1)
        highest = unit(n, scores_a, highest, scores_b)
        post(n)

        @pl.when(n >= LAG)
        def _():
            relay(n - LAG)

        fetch_q(n + 2)
        highest = unit(n + 1, scores_b, highest, scores_a)
        post(n + 1)

        @pl.when(n + 1 >= LAG)
        def _():
            relay(n + 1 - LAG)

        return highest

    highest = first_scores()
    highest = lax.fori_loop(0, views - 1, two_steps, highest)
    last = steps - 2
    fetch_q(last + 1)
    highest = unit(last, scores_a, highest, scores_b)
    post(last)
    wo_arrival = remote(wo.at[other, mine], wo.at[other, mine], wo_sem, (0,), {"tok": other})
    wo_arrival.wait_recv()
    wo_swap = remote(wo.at[other, mine], wo.at[other, mine], wo_sem, (1,), {"obj": twin})
    wo_swap.start()
    unit(last + 1, scores_b, highest, None)
    post(last + 1)

    def relay_rest(n, carry):
        relay(n)
        return carry

    lax.fori_loop(last - LAG, steps, relay_rest, 0)

    remote(wo.at[other, theirs], wo.at[other, theirs], wo_sem, (1,), {"obj": twin}).wait_recv()

    columns = width // CHUNK

    def join(slot, ab):
        at_rows = pl.ds(pl.multiple_of(ab * SUB, SUB), SUB)
        gathered[...] = att[ab, :, :, half_of[slot]].reshape(2 * views * HS, SUB).T
        for c in range(columns):
            at = slice(c * CHUNK, (c + 1) * CHUNK)
            whole = wo[:, :, at].reshape(2 * views * HS, CHUNK)
            middle[slot, at_rows, at] = rows_in[slot, at_rows, at].astype(F32) + jnp.dot(
                gathered[...], whole, preferred_element_type=F32
            )
        normed[2 * slot + ab] = normalize(middle[slot, at_rows]).astype(BF16)

    def units(block, target):
        wide = 2 * CHUNK
        for c in range(hidden.shape[1] // wide):
            at = slice(c * wide, (c + 1) * wide)
            linear = jnp.dot(block, vu[:, at], preferred_element_type=F32)
            gating = jnp.dot(block, gu[:, at], preferred_element_type=F32)
            target[:, at] = (linear * gelu(gating)).astype(BF16)

    def part_copy(ab, c):
        return remote(part_out.at[ab, c], part_in.at[ab, c], part_sem, (ab, c), {"tok": other})

    def for_partner(ab, carry):
        def one(n, carry):
            relay_arrival(ab * views + n).wait_recv()
            return carry

        lax.fori_loop(0, views, one, 0)
        join(1, ab)
        units(normed[2 + ab], hidden.at[first])
        for c in range(columns):
            at = slice(c * CHUNK, (c + 1) * CHUNK)
            part = jnp.dot(hidden[first], dw[:, at], preferred_element_type=F32)
            part_out[ab, c] = part.astype(BF16)
            part_copy(ab, c).start()
        return carry

    for item in loads[6:]:
        item.wait()
    lax.fori_loop(0, 2, for_partner, 0)

    def join_own(ab, carry):
        join(0, ab)
        return carry

    lax.fori_loop(0, 2, join_own, 0)
    units(normed[:2].reshape(rows, width), hidden)

    def keep_part(c, carry):
        at = pl.ds(pl.multiple_of(c * CHUNK, CHUNK), CHUNK)
        part_own[c] = jnp.dot(hidden[...], dw[:, at], preferred_element_type=F32)
        return carry

    lax.fori_loop(0, columns, keep_part, 0)

    for ab in range(2):
        for c in range(columns):
            part_copy(ab, c).wait_recv()
            at = slice(c * CHUNK, (c + 1) * CHUNK)
            total = middle[0, sub[ab], at] + part_own[c, sub[ab]] + part_in[ab, c].astype(F32)
            out_ref[sub[ab], at] = total.astype(BF16)

    for item in lat_copies:
        item.wait_send()
    wo_across.wait_send()
    wo_swap.wait_send()

    def drain(d, carry):
        for slot in range(2):
            for ab in range(2):
                kv_copy(2 * slot + ab, d).wait_send()
                q_copy(slot, ab, d).wait_send()
        for ab in range(2):
            att_copy(ab * views + d - 1).wait_send()
        return carry

    lax.fori_loop(1, views, drain, 0)

    def drain_relays(n, carry):
        relay_copy(n).wait_send()
        return carry

    lax.fori_loop(0, steps, drain_relays, 0)

    def drain_parts(c, carry):
        for ab in range(2):
            part_copy(ab, c).wait_send()
        return carry

    lax.fori_loop(0, columns, drain_parts, 0)


def by_heads(latents, *weights):
    views = lax.axis_size("view")
    width = latents.shape[-1]
    stream = latents.reshape(-1, width)
    rows = stream.shape[0]
    head_width, units = weights[0].shape[1], weights[4].shape[1]
    columns = width // CHUNK
    dma = pltpu.SemaphoreType.DMA
    scratch = [
        pltpu.VMEM((2, rows, width), BF16),
        pltpu.VMEM((width, head_width), BF16),
        pltpu.VMEM((width, head_width), BF16),
        pltpu.VMEM((width, head_width), BF16),
        pltpu.VMEM((2, head_width, width), BF16),
        pltpu.VMEM((width, units), BF16),
        pltpu.VMEM((width, units), BF16),
        pltpu.VMEM((units, width), BF16),
        pltpu.VMEM((4, SUB, width), BF16),
        pltpu.VMEM((4, views, HS, SUB), BF16),
        pltpu.VMEM((4, views, 2, HS, SUB), BF16),
        pltpu.VMEM((2, views, 2, HS, SUB), BF16),
        pltpu.VMEM((4, views, 2, HS, SUB), BF16),
        pltpu.VMEM((2, views, rows, HS), BF16),
        pltpu.VMEM((2, views, HS + ONES, rows), BF16),
        pltpu.VMEM((2 * views, rows, rows), F32),
        pltpu.VMEM((2 * views, rows, rows), F32),
        pltpu.VMEM((2, views, 2, HS, SUB), BF16),
        pltpu.VMEM((2, 2, views, 2, HS, SUB), BF16),
        pltpu.VMEM((SUB, 2 * head_width), BF16),
        pltpu.VMEM((2, rows, width), F32),
        pltpu.VMEM((rows, units), BF16),
        pltpu.VMEM((columns, rows, CHUNK), F32),
        pltpu.VMEM((2, columns, SUB, CHUNK), BF16),
        pltpu.VMEM((2, columns, SUB, CHUNK), BF16),
        dma((9,)),
        dma((2, 2)),
        dma((2, 4, views)),
        dma((2, 4, views)),
        dma((2, 2)),
        dma((2, 2, views + 1)),
        dma((2, 2, views + 1)),
        dma((2, 2, columns)),
    ]
    result = pl.pallas_call(
        functools.partial(block_kernel, views),
        out_shape=jax.ShapeDtypeStruct((rows, width), BF16),
        in_specs=[ANY] * 8,
        out_specs=pl.BlockSpec(memory_space=pltpu.VMEM),
        scratch_shapes=scratch,
        compiler_params=pltpu.CompilerParams(
            collective_id=0, has_side_effects=True, vmem_limit_bytes=56 * 1024 * 1024
        ),
        name="block",
    )(stream, *weights)
    return result.reshape(latents.shape)


def by_ring(
    latents,
    query_weight,
    key_weight,
    value_weight,
    output_weight,
    value_units,
    gate_units,
    down_weight,
):
    stream = latents.astype(jnp.float32)
    normed = normalize(stream).astype(jnp.bfloat16)
    joined = jnp.concatenate([query_weight, key_weight, value_weight], 1)
    projected = jnp.dot(
        lax.all_gather(normed, "tok", axis=0, tiled=True),
        joined,
        preferred_element_type=jnp.float32,
    ).astype(jnp.bfloat16)
    head_width = query_weight.shape[1]
    queries = projected[..., :head_width]
    key_part = projected[..., head_width : 2 * head_width]
    value_part = projected[..., 2 * head_width :]
    length_all, local_views, objects = (queries.shape[0], queries.shape[1], queries.shape[2])
    head_count = head_width // HS
    query_rows = length_all * local_views
    queries_flat = queries.reshape(query_rows, objects, head_count, HS)
    factor = HS ** (-0.5)

    def attend(states, key_block, value_block):
        key_rows = key_block.shape[0]

        def one_view(counter, inner):
            highest, totals, blended = inner
            key_view = lax.dynamic_index_in_dim(key_block, counter, 1, keepdims=False).reshape(
                key_rows, objects, head_count, HS
            )
            value_view = lax.dynamic_index_in_dim(value_block, counter, 1, keepdims=False).reshape(
                key_rows, objects, head_count, HS
            )
            scores = (
                jnp.einsum(
                    "ibhe,jbhe->bhij", queries_flat, key_view, preferred_element_type=jnp.float32
                )
                * factor
            )
            newest = jnp.maximum(highest, jnp.max(scores, -1))
            shrink = jnp.exp(highest - newest)
            weights = jnp.exp(scores - newest[..., None])
            totals = totals * shrink + jnp.sum(weights, -1)
            update = jnp.einsum(
                "bhij,jbhe->bhie",
                weights.astype(jnp.bfloat16),
                value_view,
                preferred_element_type=jnp.float32,
            )
            blended = blended * shrink[..., None] + update
            return (newest, totals, blended)

        return lax.fori_loop(0, key_block.shape[1], one_view, states)

    start_state = (
        jnp.full((objects, head_count, query_rows), -1e30, jnp.float32),
        jnp.zeros((objects, head_count, query_rows), jnp.float32),
        jnp.zeros((objects, head_count, query_rows, HS), jnp.float32),
    )
    stacked = jnp.stack([key_part, value_part])
    states = attend(start_state, key_part, value_part)

    def rotate(counter, bundle):
        inner, buffer_kv = bundle
        buffer_kv = passed_along(buffer_kv, "view", 1)
        return (attend(inner, buffer_kv[0], buffer_kv[1]), buffer_kv)

    states, stacked = lax.fori_loop(0, lax.axis_size("view") - 1, rotate, (states, stacked))
    highest, totals, blended = states
    attended = (blended / totals[..., None]).transpose(2, 0, 1, 3)
    attended = attended.reshape(length_all, local_views, objects, head_width).astype(jnp.bfloat16)
    full_output = lax.all_gather(output_weight, "tok", axis=0, tiled=True)
    own_rows = lax.all_to_all(attended, "tok", split_axis=0, concat_axis=3, tiled=True)
    groups = lax.axis_size("tok")
    grouped = own_rows.reshape(
        own_rows.shape[0], own_rows.shape[1], own_rows.shape[2], groups, head_width
    )
    weight_groups = full_output.reshape(groups, head_width, full_output.shape[1])
    group_parts = jnp.einsum(
        "rvbgc,gcd->rvbgd", grouped, weight_groups, preferred_element_type=jnp.float32
    ).astype(jnp.bfloat16)
    attention_out = jnp.sum(group_parts.astype(jnp.float32), 3)
    middle = stream + attention_out
    normed_two = normalize(middle).astype(jnp.bfloat16)
    gathered = lax.all_gather(normed_two, "tok", axis=0, tiled=True)
    linear = jnp.dot(gathered, value_units, preferred_element_type=jnp.float32)
    gating = jnp.dot(gathered, gate_units, preferred_element_type=jnp.float32)
    hidden = (linear * jax.nn.gelu(gating)).astype(jnp.bfloat16)
    feed_out = lax.psum_scatter(
        jnp.dot(hidden, down_weight, preferred_element_type=jnp.float32).astype(jnp.bfloat16),
        "tok",
        scatter_dimension=0,
        tiled=True,
    ).astype(jnp.float32)
    return (middle + feed_out).astype(jnp.bfloat16)


def on_device(latents, query_weight, *weights):
    rows, width = latents.shape[0], latents.shape[-1]
    head_width, unit_width = query_weight.shape[1], weights[3].shape[1]
    fits = (
        latents.shape[1] == 1
        and latents.shape[2] == 1
        and head_width == lax.axis_size("view") * HS
        and lax.axis_size("tok") == 2
        and lax.axis_size("obj") == 2
        and rows == 2 * SUB
        and width % CHUNK == 0
        and unit_width % (2 * CHUNK) == 0
    )
    if fits:
        return by_heads(latents, query_weight, *weights)
    return by_ring(latents, query_weight, *weights)


def solution(mesh):
    return jax.shard_map(
        on_device,
        mesh=mesh,
        in_specs=(
            P("tok", "view", "obj", None),
            P(None, "tok"),
            P(None, "tok"),
            P(None, "tok"),
            P("tok", None),
            P(None, "tok"),
            P(None, "tok"),
            P("tok", None),
        ),
        out_specs=P("tok", "view", "obj", None),
        check_vma=False,
    )
```

```python
import functools
import math

import jax
import jax.numpy as jnp
from jax import lax
from jax.experimental import pallas as pl
from jax.experimental.pallas import tpu as pltpu
from jax.sharding import PartitionSpec as P

HS = 64
ONES = 16
CHUNK = 256
SUB = 128
LAG = 5
MESH = pl.DeviceIdType.MESH
ANY = pl.BlockSpec(memory_space=pl.ANY)
F32, BF16 = jnp.float32, jnp.bfloat16


epsilon = 1e-05


def passed_along(block, axis, distance):
    devices = range(lax.axis_size(axis))
    route = [((i - distance) % len(devices), i) for i in devices]
    return lax.ppermute(block, axis, route)


def normalize(stream):
    average = jnp.mean(stream, -1, keepdims=True)
    centered = stream - average
    spread = jnp.mean(centered * centered, -1, keepdims=True)
    return centered * lax.rsqrt(spread + epsilon)


def gelu(v):
    return 0.5 * v * (1.0 + jnp.tanh(math.sqrt(2.0 / math.pi) * (v + 0.044715 * (v * v * v))))


def block_kernel(
    views,
    latents,
    query_weight,
    key_weight,
    value_weight,
    output_weight,
    value_units,
    gate_units,
    down_weight,
    out_ref,
    rows_in,
    wq,
    wk,
    wv,
    wo,
    vu,
    gu,
    dw,
    normed,
    send_q,
    send_kv,
    q_all,
    kv_all,
    keys,
    vals,
    scores_a,
    scores_b,
    staged,
    att,
    gathered,
    middle,
    hidden,
    part_own,
    part_out,
    part_in,
    load_sem,
    lat_sem,
    kv_sem,
    q_sem,
    wo_sem,
    att_sem,
    relay_sem,
    part_sem,
):
    view, tok, obj = lax.axis_index("view"), lax.axis_index("tok"), lax.axis_index("obj")
    other, twin = 1 - tok, 1 - obj
    width = rows_in.shape[2]
    rows = 2 * SUB
    half_of = (tok, other)
    first, second = pl.ds(0, SUB), pl.ds(SUB, SUB)
    sub = (first, second)

    def load(number, source, target):
        return pltpu.make_async_copy(source, target, load_sem.at[number])

    loads = [
        load(0, latents.at[first], rows_in.at[0, first]),
        load(1, latents.at[second], rows_in.at[0, second]),
        load(2, key_weight, wk),
        load(3, value_weight, wv),
        load(4, query_weight, wq),
        load(5, output_weight, wo.at[tok]),
        load(6, value_units, vu),
        load(7, gate_units, gu),
        load(8, down_weight, dw),
    ]
    for item in loads[:5]:
        item.start()

    barrier = pltpu.get_barrier_semaphore()
    for d in range(1, views):
        pl.semaphore_signal(
            barrier, inc=1, device_id={"view": lax.rem(view + d, views)}, device_id_type=MESH
        )
    pl.semaphore_signal(barrier, inc=1, device_id={"tok": other}, device_id_type=MESH)
    pl.semaphore_signal(barrier, inc=1, device_id={"obj": twin}, device_id_type=MESH)

    def remote(source, target, sems, index, device):
        return pltpu.make_async_remote_copy(
            src_ref=source,
            dst_ref=target,
            send_sem=sems.at[(0,) + index],
            recv_sem=sems.at[(1,) + index],
            device_id=device,
            device_id_type=MESH,
        )

    lat_copies = [
        remote(rows_in.at[0, sub[ab]], rows_in.at[1, sub[ab]], lat_sem, (ab,), {"tok": other})
        for ab in range(2)
    ]
    far_first = sorted(range(1, views), key=lambda d: abs(d - views // 2))

    def kv_copy(chunk, d):
        peer = lax.rem(view + d, views)
        return remote(
            send_kv.at[chunk, peer], kv_all.at[chunk, view], kv_sem, (chunk, d), {"view": peer}
        )

    def q_copy(slot, ab, d):
        peer, chunk = lax.rem(view + d, views), 2 * slot + ab
        return remote(
            send_q.at[chunk, peer],
            q_all.at[ab, view, half_of[slot]],
            q_sem,
            (chunk, d),
            {"view": peer},
        )

    def kv_arrival(chunk, d):
        source = lax.rem(view - d + views, views)
        return remote(
            send_kv.at[chunk, source], kv_all.at[chunk, source], kv_sem, (chunk, d), {"view": source}
        )

    def q_arrival(slot, ab, d):
        source, chunk = lax.rem(view - d + views, views), 2 * slot + ab
        return remote(
            send_q.at[chunk, source],
            q_all.at[ab, source, half_of[slot]],
            q_sem,
            (chunk, d),
            {"view": source},
        )

    def level(slot, ab):
        normed[2 * slot + ab] = normalize(rows_in[slot, sub[ab]].astype(F32)).astype(BF16)

    def project(chunk, weight):
        return jnp.dot(normed[chunk], weight[...], preferred_element_type=F32)

    def turned(projected):
        return projected.astype(BF16).T.reshape(views, HS, SUB)

    def spread_kv(chunk):
        send_kv[chunk, :, 0] = turned(project(chunk, wk))
        send_kv[chunk, :, 1] = turned(project(chunk, wv))
        for d in far_first:
            kv_copy(chunk, d).start()
        kv_all[chunk, view] = send_kv[chunk, view]

    def make_q(chunk):
        send_q[chunk] = turned(project(chunk, wq) * (HS**-0.5 * math.log2(math.e)))

    def spread_q(slot, ab):
        for d in range(views - 1, 0, -1):
            q_copy(slot, ab, d).start()
        q_all[ab, view, half_of[slot]] = send_q[2 * slot + ab, view]

    loads[0].wait()
    level(0, 0)
    loads[1].wait()
    pl.semaphore_wait(barrier, views + 1)
    for item in lat_copies:
        item.start()
    loads[2].wait()
    loads[3].wait()
    spread_kv(0)
    level(0, 1)
    spread_kv(1)
    loads[4].wait()
    for item in loads[5:]:
        item.start()
    make_q(0)
    make_q(1)

    lat_copies[0].wait_recv()
    level(1, 0)
    spread_kv(2)
    make_q(2)
    lat_copies[1].wait_recv()
    loads[5].wait()
    share = wo.shape[1] // 2
    mine, theirs = pl.ds(obj * share, share), pl.ds(twin * share, share)
    wo_across = remote(wo.at[tok, mine], wo.at[tok, mine], wo_sem, (0,), {"tok": other})
    wo_across.start()
    level(1, 1)
    spread_kv(3)
    make_q(3)

    vals[:, :, HS:, :] = jnp.ones((2, views, ONES, rows), BF16)

    def prepare(slot, ab):
        chunk = 2 * slot + ab

        def one(d, carry):
            source = lax.rem(view - d + views, views)

            @pl.when(d > 0)
            def _():
                kv_arrival(chunk, d).wait_recv()

            keys[slot, source, sub[ab]] = kv_all[chunk, source, 0].T
            vals[slot, source, :HS, sub[ab]] = kv_all[chunk, source, 1]
            return carry

        lax.fori_loop(0, views, one, 0)

    for chunk in range(3):
        prepare(chunk // 2, chunk % 2)

    def left(d, carry):
        kv_copy(3, d).wait_send()
        return carry

    lax.fori_loop(1, views, left, 0)
    spread_q(0, 0)
    spread_q(1, 0)
    prepare(1, 1)

    def left_too(d, carry):
        for slot in range(2):
            q_copy(slot, 0, d).wait_send()
        return carry

    lax.fori_loop(1, views, left_too, 0)
    spread_q(0, 1)
    spread_q(1, 1)

    steps = 2 * views
    blocks = [(slot, number) for slot in range(2) for number in range(views)]

    def place(n):
        later = n - 2
        ab = jnp.where(later < 0, n, later // (views - 1))
        turn = jnp.where(later < 0, views, lax.rem(later + views - 1, views - 1) + 1)
        return ab, turn, lax.rem(view + turn, views), lax.rem(view - turn + views, views)

    def fetch_q(n):
        ab, turn, target, _ = place(n)

        @pl.when(turn != views)
        def _():
            for slot in range(2):
                q_arrival(slot, ab, views - turn).wait_recv()

    def att_copy(ab, turn):
        target = lax.rem(view + turn, views)
        return remote(
            staged.at[ab, target], att.at[ab, tok, view], att_sem, (ab, turn), {"view": target}
        )

    def att_arrival(n):
        ab, turn, _, source = place(n)
        return remote(
            staged.at[ab, source], att.at[ab, tok, source], att_sem, (ab, turn), {"view": source}
        )

    def relay_copy(ab, turn):
        source = lax.rem(view - turn + views, views)
        block = att.at[ab, tok, source]
        return remote(block, block, relay_sem, (ab, turn), {"tok": other})

    def relay_arrival(ab, turn):
        source = lax.rem(view - turn + views, views)
        block = att.at[ab, other, source]
        return remote(block, block, relay_sem, (ab, turn), {"tok": other})

    def score(n, buffer, number):
        ab, _, target, _ = place(n)
        queries = jnp.concatenate([q_all[ab, target, 0], q_all[ab, target, 1]], 1)
        found = jnp.dot(keys[blocks[number]], queries, preferred_element_type=F32)
        buffer[number] = found
        return jnp.max(found, 0, keepdims=True)

    def blend(buffer, highest, number):
        weights = jnp.exp2(buffer[number] - highest).astype(BF16)
        return jnp.dot(vals[blocks[number]], weights, preferred_element_type=F32)

    def unit(n, current, highest, following):
        blended = jnp.zeros((HS + ONES, rows), F32)
        upcoming = jnp.full((1, rows), -1e30, F32)
        for number in range(steps):
            if following is not None:
                upcoming = jnp.maximum(upcoming, score(n + 1, following, number))
            blended = blended + blend(current, highest, number)
        result = (blended[:HS] / blended[HS : HS + 1]).astype(BF16)
        ab, _, target, _ = place(n)
        staged[ab, target, 0] = result[:, :SUB]
        staged[ab, target, 1] = result[:, SUB:]
        return upcoming

    def post(n):
        ab, turn, target, _ = place(n)

        @pl.when(turn != views)
        def _():
            att_copy(ab, turn).start()

        @pl.when(turn == views)
        def _():
            att[ab, tok, view] = staged[ab, view]

    def relay(n):
        ab, turn, _, _ = place(n)

        @pl.when(turn != views)
        def _():
            att_arrival(n).wait_recv()

        relay_copy(ab, turn).start()

    def first_scores():
        fetch_q(0)
        highest = jnp.full((1, rows), -1e30, F32)
        for number in range(steps):
            highest = jnp.maximum(highest, score(0, scores_a, number))
        return highest

    wo_arrival = remote(wo.at[other, mine], wo.at[other, mine], wo_sem, (0,), {"tok": other})
    wo_swap = remote(wo.at[other, mine], wo.at[other, mine], wo_sem, (1,), {"obj": twin})

    def two_steps(i, highest):
        n = 2 * i

        @pl.when(i == views // 2)
        def _():
            wo_arrival.wait_recv()
            wo_swap.start()

        fetch_q(n + 1)
        highest = unit(n, scores_a, highest, scores_b)
        post(n)

        @pl.when(n >= LAG)
        def _():
            relay(n - LAG)

        fetch_q(n + 2)
        highest = unit(n + 1, scores_b, highest, scores_a)
        post(n + 1)

        @pl.when(n + 1 >= LAG)
        def _():
            relay(n + 1 - LAG)

        return highest

    def relays(start, stop):
        def one(n, carry):
            relay(n)
            return carry

        lax.fori_loop(start, stop, one, 0)

    highest = first_scores()
    highest = lax.fori_loop(0, views - 1, two_steps, highest)
    last = steps - 2
    fetch_q(last + 1)
    highest = unit(last, scores_a, highest, scores_b)
    post(last)
    relay(last - LAG)
    unit(last + 1, scores_b, highest, None)
    post(last + 1)
    relay(last + 1 - LAG)

    columns = width // CHUNK

    def join(slot, ab):
        at_rows = pl.ds(pl.multiple_of(ab * SUB, SUB), SUB)
        gathered[...] = att[ab, :, :, half_of[slot]].reshape(2 * views * HS, SUB).T
        for c in range(columns):
            at = slice(c * CHUNK, (c + 1) * CHUNK)
            whole = wo[:, :, at].reshape(2 * views * HS, CHUNK)
            middle[slot, at_rows, at] = rows_in[slot, at_rows, at].astype(F32) + jnp.dot(
                gathered[...], whole, preferred_element_type=F32
            )
        normed[2 * slot + ab] = normalize(middle[slot, at_rows]).astype(BF16)

    def units(block, target):
        wide = 2 * CHUNK
        for c in range(hidden.shape[1] // wide):
            at = slice(c * wide, (c + 1) * wide)
            linear = jnp.dot(block, vu[:, at], preferred_element_type=F32)
            gating = jnp.dot(block, gu[:, at], preferred_element_type=F32)
            target[:, at] = (linear * gelu(gating)).astype(BF16)

    def part_copy(ab, c):
        return remote(part_out.at[ab, c], part_in.at[ab, c], part_sem, (ab, c), {"tok": other})

    def relayed(ab):
        def one(n, carry):
            relay_arrival(ab, n).wait_recv()
            return carry

        lax.fori_loop(1, views + 1, one, 0)

    def down(c):
        at = slice(c * CHUNK, (c + 1) * CHUNK)
        return jnp.dot(hidden[...], dw[:, at], preferred_element_type=F32)

    def send_parts(ab):
        for c in range(columns):
            part_out[ab, c] = down(c).astype(BF16)
        for c in range(columns):
            part_copy(ab, c).start()

    def keep_parts(ab):
        for c in range(columns):
            part_own[ab, c] = down(c)

    for item in loads[6:]:
        item.wait()
    remote(wo.at[other, theirs], wo.at[other, theirs], wo_sem, (1,), {"obj": twin}).wait_recv()
    relayed(0)
    join(1, 0)
    relays(2 * views - LAG, 2 * views)
    units(normed[2], hidden)
    send_parts(0)
    relayed(1)
    join(1, 1)
    units(normed[3], hidden)
    send_parts(1)
    for ab in range(2):
        join(0, ab)
        units(normed[ab], hidden)
        keep_parts(ab)

    for ab in range(2):
        for c in range(columns):
            part_copy(ab, c).wait_recv()
            at = slice(c * CHUNK, (c + 1) * CHUNK)
            total = middle[0, sub[ab], at] + part_own[ab, c] + part_in[ab, c].astype(F32)
            out_ref[sub[ab], at] = total.astype(BF16)

    for item in lat_copies:
        item.wait_send()
    wo_across.wait_send()
    wo_swap.wait_send()

    def drain(d, carry):
        for slot in range(2):
            for ab in range(2):
                if 2 * slot + ab < 3:
                    kv_copy(2 * slot + ab, d).wait_send()
            q_copy(slot, 1, d).wait_send()
        for ab in range(2):
            att_copy(ab, d).wait_send()
        return carry

    lax.fori_loop(1, views, drain, 0)

    def drain_relays(n, carry):
        for ab in range(2):
            relay_copy(ab, n).wait_send()
        return carry

    lax.fori_loop(1, views + 1, drain_relays, 0)

    def drain_parts(c, carry):
        for ab in range(2):
            part_copy(ab, c).wait_send()
        return carry

    lax.fori_loop(0, columns, drain_parts, 0)


def by_heads(latents, *weights):
    views = lax.axis_size("view")
    width = latents.shape[-1]
    stream = latents.reshape(-1, width)
    rows = stream.shape[0]
    head_width, units = weights[0].shape[1], weights[4].shape[1]
    columns = width // CHUNK
    dma = pltpu.SemaphoreType.DMA
    scratch = [
        pltpu.VMEM((2, rows, width), BF16),
        pltpu.VMEM((width, head_width), BF16),
        pltpu.VMEM((width, head_width), BF16),
        pltpu.VMEM((width, head_width), BF16),
        pltpu.VMEM((2, head_width, width), BF16),
        pltpu.VMEM((width, units), BF16),
        pltpu.VMEM((width, units), BF16),
        pltpu.VMEM((units, width), BF16),
        pltpu.VMEM((4, SUB, width), BF16),
        pltpu.VMEM((4, views, HS, SUB), BF16),
        pltpu.VMEM((4, views, 2, HS, SUB), BF16),
        pltpu.VMEM((2, views, 2, HS, SUB), BF16),
        pltpu.VMEM((4, views, 2, HS, SUB), BF16),
        pltpu.VMEM((2, views, rows, HS), BF16),
        pltpu.VMEM((2, views, HS + ONES, rows), BF16),
        pltpu.VMEM((2 * views, rows, rows), F32),
        pltpu.VMEM((2 * views, rows, rows), F32),
        pltpu.VMEM((2, views, 2, HS, SUB), BF16),
        pltpu.VMEM((2, 2, views, 2, HS, SUB), BF16),
        pltpu.VMEM((SUB, 2 * head_width), BF16),
        pltpu.VMEM((2, rows, width), F32),
        pltpu.VMEM((SUB, units), BF16),
        pltpu.VMEM((2, columns, SUB, CHUNK), F32),
        pltpu.VMEM((2, columns, SUB, CHUNK), BF16),
        pltpu.VMEM((2, columns, SUB, CHUNK), BF16),
        dma((9,)),
        dma((2, 2)),
        dma((2, 4, views)),
        dma((2, 4, views)),
        dma((2, 2)),
        dma((2, 2, views + 1)),
        dma((2, 2, views + 1)),
        dma((2, 2, columns)),
    ]
    result = pl.pallas_call(
        functools.partial(block_kernel, views),
        out_shape=jax.ShapeDtypeStruct((rows, width), BF16),
        in_specs=[ANY] * 8,
        out_specs=pl.BlockSpec(memory_space=pltpu.VMEM),
        scratch_shapes=scratch,
        compiler_params=pltpu.CompilerParams(
            collective_id=0, has_side_effects=True, vmem_limit_bytes=56 * 1024 * 1024
        ),
        name="block",
    )(stream, *weights)
    return result.reshape(latents.shape)


def by_ring(
    latents,
    query_weight,
    key_weight,
    value_weight,
    output_weight,
    value_units,
    gate_units,
    down_weight,
):
    stream = latents.astype(jnp.float32)
    normed = normalize(stream).astype(jnp.bfloat16)
    joined = jnp.concatenate([query_weight, key_weight, value_weight], 1)
    projected = jnp.dot(
        lax.all_gather(normed, "tok", axis=0, tiled=True),
        joined,
        preferred_element_type=jnp.float32,
    ).astype(jnp.bfloat16)
    head_width = query_weight.shape[1]
    queries = projected[..., :head_width]
    key_part = projected[..., head_width : 2 * head_width]
    value_part = projected[..., 2 * head_width :]
    length_all, local_views, objects = (queries.shape[0], queries.shape[1], queries.shape[2])
    head_count = head_width // HS
    query_rows = length_all * local_views
    queries_flat = queries.reshape(query_rows, objects, head_count, HS)
    factor = HS ** (-0.5)

    def attend(states, key_block, value_block):
        key_rows = key_block.shape[0]

        def one_view(counter, inner):
            highest, totals, blended = inner
            key_view = lax.dynamic_index_in_dim(key_block, counter, 1, keepdims=False).reshape(
                key_rows, objects, head_count, HS
            )
            value_view = lax.dynamic_index_in_dim(value_block, counter, 1, keepdims=False).reshape(
                key_rows, objects, head_count, HS
            )
            scores = (
                jnp.einsum(
                    "ibhe,jbhe->bhij", queries_flat, key_view, preferred_element_type=jnp.float32
                )
                * factor
            )
            newest = jnp.maximum(highest, jnp.max(scores, -1))
            shrink = jnp.exp(highest - newest)
            weights = jnp.exp(scores - newest[..., None])
            totals = totals * shrink + jnp.sum(weights, -1)
            update = jnp.einsum(
                "bhij,jbhe->bhie",
                weights.astype(jnp.bfloat16),
                value_view,
                preferred_element_type=jnp.float32,
            )
            blended = blended * shrink[..., None] + update
            return (newest, totals, blended)

        return lax.fori_loop(0, key_block.shape[1], one_view, states)

    start_state = (
        jnp.full((objects, head_count, query_rows), -1e30, jnp.float32),
        jnp.zeros((objects, head_count, query_rows), jnp.float32),
        jnp.zeros((objects, head_count, query_rows, HS), jnp.float32),
    )
    stacked = jnp.stack([key_part, value_part])
    states = attend(start_state, key_part, value_part)

    def rotate(counter, bundle):
        inner, buffer_kv = bundle
        buffer_kv = passed_along(buffer_kv, "view", 1)
        return (attend(inner, buffer_kv[0], buffer_kv[1]), buffer_kv)

    states, stacked = lax.fori_loop(0, lax.axis_size("view") - 1, rotate, (states, stacked))
    highest, totals, blended = states
    attended = (blended / totals[..., None]).transpose(2, 0, 1, 3)
    attended = attended.reshape(length_all, local_views, objects, head_width).astype(jnp.bfloat16)
    full_output = lax.all_gather(output_weight, "tok", axis=0, tiled=True)
    own_rows = lax.all_to_all(attended, "tok", split_axis=0, concat_axis=3, tiled=True)
    groups = lax.axis_size("tok")
    grouped = own_rows.reshape(
        own_rows.shape[0], own_rows.shape[1], own_rows.shape[2], groups, head_width
    )
    weight_groups = full_output.reshape(groups, head_width, full_output.shape[1])
    group_parts = jnp.einsum(
        "rvbgc,gcd->rvbgd", grouped, weight_groups, preferred_element_type=jnp.float32
    ).astype(jnp.bfloat16)
    attention_out = jnp.sum(group_parts.astype(jnp.float32), 3)
    middle = stream + attention_out
    normed_two = normalize(middle).astype(jnp.bfloat16)
    gathered = lax.all_gather(normed_two, "tok", axis=0, tiled=True)
    linear = jnp.dot(gathered, value_units, preferred_element_type=jnp.float32)
    gating = jnp.dot(gathered, gate_units, preferred_element_type=jnp.float32)
    hidden = (linear * jax.nn.gelu(gating)).astype(jnp.bfloat16)
    feed_out = lax.psum_scatter(
        jnp.dot(hidden, down_weight, preferred_element_type=jnp.float32).astype(jnp.bfloat16),
        "tok",
        scatter_dimension=0,
        tiled=True,
    ).astype(jnp.float32)
    return (middle + feed_out).astype(jnp.bfloat16)


def on_device(latents, query_weight, *weights):
    rows, width = latents.shape[0], latents.shape[-1]
    head_width, unit_width = query_weight.shape[1], weights[3].shape[1]
    fits = (
        latents.shape[1] == 1
        and latents.shape[2] == 1
        and head_width == lax.axis_size("view") * HS
        and lax.axis_size("tok") == 2
        and lax.axis_size("obj") == 2
        and rows == 2 * SUB
        and width % CHUNK == 0
        and unit_width % (2 * CHUNK) == 0
    )
    if fits:
        return by_heads(latents, query_weight, *weights)
    return by_ring(latents, query_weight, *weights)


def solution(mesh):
    return jax.shard_map(
        on_device,
        mesh=mesh,
        in_specs=(
            P("tok", "view", "obj", None),
            P(None, "tok"),
            P(None, "tok"),
            P(None, "tok"),
            P("tok", None),
            P(None, "tok"),
            P(None, "tok"),
            P("tok", None),
        ),
        out_specs=P("tok", "view", "obj", None),
        check_vma=False,
    )
```
